32 devices in a mesh: gx: 4 (over z), gy: 2 (over y), gz: 4 (over x, core).
Axes of the slice: x: 2, y: 2, z: 4, core: 2. Of those that a mesh axis runs over, the one named last changes fastest.
Arguments:
- populations: float32 [27, 16, 16, 512], P(None, 'gx', 'gy', 'gz'), may hold values from 0.85 to 1.15
- coarse_populations: float32 [27, 32, 8, 256], P(None, 'gx', 'gy', 'gz'), may hold values from 0.85 to 1.15
- fluid_mask: int32 [16, 16, 512], P('gx', 'gy', 'gz'), may hold values 0 or 1
- inflow: float32 [8, 256], P('gy', 'gz'), may hold values from 0.02 to 0.08
- part_dest: int32 [4, 2, 4, 256, 1], P('gx', 'gy', 'gz'), may hold values from 0 to 3; in each aligned block of 256 rows (0 to 255, 256 to 511, ..., all dimensions but the last counted through in order) at most 128 rows name the same one
- part_cell: int32 [4, 2, 4, 256], P('gx', 'gy', 'gz'), may hold values from 0 to 2942, as said below
- part_vel: float32 [4, 2, 4, 3, 256], P('gx', 'gy', 'gz'), may hold values from -0.3 to 0.3
- part_frac: float32 [4, 2, 4, 3, 256], P('gx', 'gy', 'gz'), may hold values from 0 to 1
- part_drag: float32 [4, 2, 4, 256], P('gx', 'gy', 'gz'), may hold values from 0.05 to 0.5
Outputs:
- fine_next: float32 [27, 16, 16, 512], P(None, 'gx', 'gy', 'gz')
- coarse_next: float32 [27, 32, 8, 256], P(None, 'gx', 'gy', 'gz')
The draws below stay inside these ranges and needn't reach their ends.
Inputs may be any that keep to these rules, and one draw needn't show every extreme that they name: `part_dest`: among the particles of one device at most 128 have the same destination. `part_cell`: ix < 3, iy < 7 and iz < 127, so that all eight corners lie in the destination block.
All inputs are finite; a program needn't handle non-finite values. No bound on the sum of `fluid_mask` on one device may be relied on, other than what follows from the above.
Results may differ from the reference program's by a relative error of at most 0.000078.
Values sent between devices are 32-bit elements; how exact they have to be, the bound alone decides.
A program may use at most 128 MiB of HBM per device.

```python
import math
import jax
import jax.numpy as jnp
import numpy as np
from jax import lax

CX = 4
CY = 8
CZ = 128
P_DEV = 256
CAP = 128
NX = 16
NY = 16
NZ = 512
LX = 32
N_GX = 4
N_GY = 2
N_GZ = 4


def draw_part_cell(key, part):
    keys = jax.random.split(jax.random.fold_in(key, 7), 3)
    shape = (N_GX, N_GY, N_GZ, P_DEV)
    cell_x = jax.random.randint(keys[0], shape, 0, CX - 1)
    cell_y = jax.random.randint(keys[1], shape, 0, CY - 1)
    cell_z = jax.random.randint(keys[2], shape, 0, CZ - 1)
    return (cell_x * CY * CZ + cell_y * CZ + cell_z).astype(jnp.int32)


def with_ends(entries, key, least, largest):
    longest = entries.shape.index(max(entries.shape))
    spots = []
    for shift in (0, 1):
        where = [jax.random.randint(jax.random.fold_in(key, axis), (), 0, length) for axis, length in enumerate(entries.shape)]
        where[longest] = (where[longest] + shift) % entries.shape[longest]
        spots.append(tuple(where))
    return entries.at[spots[0]].set(least).at[spots[1]].set(largest)


def shard_levels(rng, shape, cuts, low, high):
    gain = 1.0
    for position, parts in cuts:
        steps = jax.random.uniform(jax.random.fold_in(jax.random.fold_in(rng, 6), position), (parts,), jnp.float32, low / len(cuts), high / len(cuts))
        gain = gain * jnp.repeat(jnp.exp(steps), shape[position] // parts).reshape((-1,) + (1,) * (len(shape) - 1 - position))
    return gain


def routed_block(rng, own, number, rows, number_of, top, most, slope):
    ranking = jax.random.permutation(rng, number_of)
    heavy_load, ordinary = shares(number_of, rows * top, most, slope, True), shares(number_of, rows * top, most, slope, False)
    places = jnp.arange(number_of)

    def named(tallies, turn):
        used = int((tallies > 0).sum())
        fixed = max(1, used // 4)
        shifted = fixed + (places - fixed + turn * (used - fixed)) % max(1, number_of - fixed)
        return jnp.zeros((number_of,), jnp.int32).at[ranking[jnp.where(places < fixed, places, shifted)]].set(jnp.asarray(tallies, jnp.int32))

    tallies = jnp.where(number % 4 == 0, named(heavy_load, number // 4), named(ordinary, number - number // 4 - 1))
    mixed = jax.random.permutation(jax.random.fold_in(own, 3), number_of)
    giver, taker = mixed[0:number_of // 2 * 2:2], mixed[1:number_of // 2 * 2:2]
    margin = jnp.minimum(tallies[giver] - 1, most - tallies[taker]) // 2
    margin = jnp.where((giver == ranking[0]) | (taker == ranking[0]) | (tallies[taker] == 0), 0, jnp.maximum(margin, 0))
    shifted = jax.random.randint(jax.random.fold_in(own, 4), (number_of // 2,), 0, 1 << 20) % (margin + 1)
    tallies = tallies.at[giver].add(-shifted).at[taker].add(shifted)
    members = jnp.searchsorted(jnp.cumsum(tallies), jnp.arange(rows * top), side="right").astype(jnp.int32)
    table = members.reshape(top, rows).T
    table = table[jax.random.permutation(jax.random.fold_in(own, 1), rows)]
    turn = jax.random.randint(jax.random.fold_in(own, 2), (rows, 1), 0, top)
    return jnp.take_along_axis(table, (jnp.arange(top)[None, :] + turn) % top, axis=1)


def shares(amount, total, bound, slope, full):
    loads = [(1 << 20) // math.isqrt(standing ** slope) + 1 for standing in range(1, amount + 1)]
    largest = bound if full else min(bound, max(-(-total // amount), total * loads[0] // sum(loads)))
    least = 1 if total - largest >= amount - 1 else 0
    counts, spare = [largest] + [least] * (amount - 1), total - largest - least * (amount - 1)
    while spare > 0:
        free = [i for i in range(1, amount) if counts[i] < largest] or [i for i in range(1, amount) if counts[i] < bound]
        whole, remaining = sum([loads[i] for i in free]), spare
        for i in free:
            more = min(bound - counts[i], max(1, remaining * loads[i] // whole), spare)
            counts[i] = counts[i] + more
            spare = spare - more
    return np.array(counts)


def noise(stream_key, shape, spread, reach, cuts=(), kind=jnp.bfloat16):
    gain = shard_levels(stream_key, shape, cuts, -0.22, 0.18) if cuts else 1.0
    values = jax.random.normal(stream_key, shape, jnp.float32) * spread * gain
    return jnp.minimum(jnp.maximum(values, -reach), reach).astype(kind)


def setup_inputs(seed: int = 0) -> dict:
    splits = jax.random.split(jax.random.key(seed), 10)
    populations = jnp.clip(0.85 + 0.29999995 * jax.random.uniform(splits[0], (27, NX, NY, NZ), jnp.float32) ** shard_levels(splits[0], (27, NX, NY, NZ), ((1, 4), (2, 2), (3, 4)), -0.2, 0.2), 0.85, 1.15)
    coarse_populations = jnp.clip(0.85 + 0.29999995 * jax.random.uniform(splits[1], (27, LX, NY // 2, NZ // 2), jnp.float32) ** shard_levels(splits[1], (27, LX, NY // 2, NZ // 2), ((1, 4), (2, 2), (3, 4)), -0.2, 0.2), 0.85, 1.15)
    fluid_mask = with_ends((jax.random.randint(splits[2], (NX, NY, NZ), 0, 8) < 7).astype(jnp.int32), jax.random.fold_in(splits[2], 1), 0, 1)
    inflow = jnp.clip(0.02 + 0.06 * jax.random.uniform(splits[3], (NY // 2, NZ // 2), jnp.float32) ** shard_levels(splits[3], (NY // 2, NZ // 2), ((0, 2), (1, 4)), -0.2, 0.2), 0.02, 0.08)
    part_dest_keys = jax.random.split(jax.random.fold_in(splits[4], 1), N_GX * N_GY * N_GZ * P_DEV // P_DEV)
    part_dest_turns = jax.random.permutation(jax.random.fold_in(splits[4], 3), N_GX * N_GY * N_GZ * P_DEV // P_DEV)
    part_dest = jax.vmap(lambda own, number: routed_block(jax.random.fold_in(splits[4], 2), own, number, P_DEV, N_GX, 1, CAP, 2))(part_dest_keys, part_dest_turns).reshape((N_GX, N_GY, N_GZ, P_DEV, 1))
    part_cell = draw_part_cell(jax.random.fold_in(splits[9], 71), 0)
    part_vel = noise(splits[6], (N_GX, N_GY, N_GZ, 3, P_DEV), 0.05, 0.3, ((0, 4), (1, 2), (2, 4)), jnp.float32)
    part_frac = jnp.clip(1.0 * jax.random.uniform(splits[7], (N_GX, N_GY, N_GZ, 3, P_DEV), jnp.float32) ** shard_levels(splits[7], (N_GX, N_GY, N_GZ, 3, P_DEV), ((0, 4), (1, 2), (2, 4)), -0.2, 0.2), 0.0, 1.0)
    part_drag = jnp.clip(jnp.exp(math.log(0.5) - 2.3025851 * jax.random.uniform(splits[8], (N_GX, N_GY, N_GZ, P_DEV), jnp.float32) ** shard_levels(splits[8], (N_GX, N_GY, N_GZ, P_DEV), ((0, 4), (1, 2), (2, 4)), -0.2, 0.2)), 0.05, 0.5)
    return {"populations": populations, "coarse_populations": coarse_populations, "fluid_mask": fluid_mask, "inflow": inflow, "part_dest": part_dest, "part_cell": part_cell, "part_vel": part_vel, "part_frac": part_frac, "part_drag": part_drag}


tau_fine = 1.3
tau_coarse = 0.9
stencil_ints = [(along_x, along_y, along_z) for along_x in (-1, 0, 1) for along_y in (-1, 0, 1) for along_z in (-1, 0, 1)]
stencil = np.array(stencil_ints, np.float32)
lattice_weights = np.array([8.0 / 27.0, 2.0 / 27.0, 1.0 / 54.0, 1.0 / 216.0], np.float32)[np.abs(stencil).sum(1).astype(np.int32)]
prolong_factor = (tau_fine - 1.0) / (2.0 * tau_coarse)
restrict_factor = 2.0 * (tau_coarse - 1.0) / tau_fine


def moments(normal):
    shape_tail = (1,) * (normal.ndim - 1)
    scaled = normal * lattice_weights.reshape((27,) + shape_tail)
    density = jnp.sum(scaled, axis=0)
    momentum = jnp.tensordot(stencil.T, scaled, axes=1, precision=lax.Precision.HIGHEST)
    return density, momentum


def equilibrium(density, velocity):
    projected = jnp.tensordot(stencil, velocity, axes=1, precision=lax.Precision.HIGHEST)
    square = jnp.sum(velocity * velocity, axis=0)
    return density * (1.0 + 3.0 * projected + 4.5 * projected * projected - 1.5 * square)


def collide(normal, fluid_ones, body_force, tau_value):
    density, momentum = moments(normal)
    safe_density = density + (1.0 - fluid_ones)
    velocity = momentum / safe_density + tau_value * body_force / safe_density
    return fluid_ones * (normal - (normal - equilibrium(safe_density, velocity)) / tau_value)


def interface(normal, factor):
    density, momentum = moments(normal)
    settled = equilibrium(density, momentum / density)
    return settled + factor * (normal - settled)


def restrict(normal):
    surface = normal[:, 0:2]
    half_y = surface.shape[2] // 2
    half_z = surface.shape[3] // 2
    summed = surface.reshape(27, 2, half_y, 2, half_z, 2).sum(axis=(1, 3, 5))
    return interface(0.125 * summed, restrict_factor)


def refine_layer(boundary):
    return jnp.repeat(jnp.repeat(boundary, 2, axis=1), 2, axis=2)


def stream(padded, collided, fluid_ones):
    extent = collided.shape[1:]
    result = []
    for number in range(27):
        shift_x, shift_y, shift_z = stencil_ints[number]
        anchor_x = 1 - shift_x
        anchor_y = 1 - shift_y
        anchor_z = 1 - shift_z
        source = padded[number, anchor_x:anchor_x + extent[0], anchor_y:anchor_y + extent[1], anchor_z:anchor_z + extent[2]]
        open_flag = padded[27, anchor_x:anchor_x + extent[0], anchor_y:anchor_y + extent[1], anchor_z:anchor_z + extent[2]]
        result.append(open_flag * source + (1.0 - open_flag) * collided[26 - number])
    return fluid_ones * jnp.stack(result)


def with_flag(boundary):
    return jnp.concatenate([boundary, jnp.ones((1,) + boundary.shape[1:], boundary.dtype)], 0)


def build_padded(collided, flags, left_layer, right_layer):
    stacked = jnp.concatenate([collided, flags[None]], 0)
    padded = jnp.pad(stacked, ((0, 0), (1, 1), (1, 1), (1, 1)))
    padded = padded.at[:, 0, 1:-1, 1:-1].set(with_flag(left_layer))
    if right_layer is None:
        padded = padded.at[:, -1].set(padded[:, -2])
    else:
        padded = padded.at[:, -1, 1:-1, 1:-1].set(with_flag(right_layer))
    return padded


def deposit(velocity_flat, cell_base, part_velocity, drag_values, fraction, stride_x, stride_y):
    corners = []
    sampled = jnp.zeros_like(part_velocity)
    for corner in range(8):
        offset_x = corner // 4
        offset_y = (corner // 2) % 2
        offset_z = corner % 2
        weight = (fraction[0] if offset_x else 1.0 - fraction[0]) * (fraction[1] if offset_y else 1.0 - fraction[1]) * (fraction[2] if offset_z else 1.0 - fraction[2])
        corner_index = cell_base + offset_x * stride_x + offset_y * stride_y + offset_z
        sampled = sampled + weight * velocity_flat[:, corner_index]
        corners.append((weight, corner_index))
    impulse = drag_values * (part_velocity - sampled)
    body_force = jnp.zeros_like(velocity_flat)
    for weight, corner_index in corners:
        body_force = body_force.at[:, corner_index].add(weight * impulse)
    return body_force


def reference(populations, coarse_populations, fluid_mask, inflow, part_dest, part_cell, part_vel, part_frac, part_drag):
    open_cells = fluid_mask.astype(jnp.float32)
    density, momentum = moments(populations)
    safe_density = density + (1.0 - open_cells)
    velocity_flat = (momentum / safe_density).reshape(3, -1)
    slab_ids = part_dest[..., 0]
    column_ids = jnp.arange(N_GY, dtype=jnp.int32)[None, :, None, None]
    row_ids = jnp.arange(N_GZ, dtype=jnp.int32)[None, None, :, None]
    local_x = part_cell // (CY * CZ)
    local_y = (part_cell // CZ) % CY
    local_z = part_cell % CZ
    global_cell = ((slab_ids * CX + local_x) * NY + column_ids * CY + local_y) * NZ + row_ids * CZ + local_z
    body_force = deposit(velocity_flat, global_cell.reshape(-1), jnp.moveaxis(part_vel, 3, 0).reshape(3, -1), part_drag.reshape(-1), jnp.moveaxis(part_frac, 3, 0).reshape(3, -1), NY * NZ, NZ)
    body_force = body_force.reshape((3,) + open_cells.shape)
    restricted = restrict(populations)
    zeros_plane = jnp.zeros_like(inflow)
    inlet = equilibrium(1.0, jnp.stack([inflow, zeros_plane, zeros_plane]))
    coarse_collided = collide(coarse_populations, 1.0, 0.0, tau_coarse)
    coarse_flags = jnp.ones(coarse_populations.shape[1:], jnp.float32)
    coarse_next = stream(build_padded(coarse_collided, coarse_flags, inlet, restricted), coarse_collided, 1.0)
    start_ghost = refine_layer(interface(coarse_populations[:, -1], prolong_factor))
    collided = collide(populations, open_cells, body_force, tau_fine)
    middle = stream(build_padded(collided, open_cells, start_ghost, None), collided, open_cells)
    late_ghost = refine_layer(interface(0.5 * (coarse_populations[:, -1] + coarse_next[:, -1]), prolong_factor))
    collided = collide(middle, open_cells, body_force, tau_fine)
    finished = stream(build_padded(collided, open_cells, late_ghost, None), collided, open_cells)
    return finished, coarse_next
```

```python
import functools

import jax
import jax.numpy as jnp
import numpy as np
from jax import lax
from jax.experimental import pallas as pl
from jax.experimental.pallas import tpu as pltpu
from jax.sharding import PartitionSpec as P

tau_fine = 1.3
tau_coarse = 0.9
stencil_ints = [
    (along_x, along_y, along_z)
    for along_x in (-1, 0, 1)
    for along_y in (-1, 0, 1)
    for along_z in (-1, 0, 1)
]
weights = [
    float(np.float32([8.0 / 27.0, 2.0 / 27.0, 1.0 / 54.0, 1.0 / 216.0][sum(map(abs, c))]))
    for c in stencil_ints
]
prolong_factor = (tau_fine - 1.0) / (2.0 * tau_coarse)
restrict_factor = 2.0 * (tau_coarse - 1.0) / tau_fine
closed = -3.0e38
groups = {
    (dim, side): [i for i, c in enumerate(stencil_ints) if c[dim] == side]
    for dim in range(3)
    for side in (-1, 1)
}
MESH = pl.DeviceIdType.MESH
HIGHEST = lax.Precision.HIGHEST


def moments(get):
    density = None
    sums = [None, None, None]
    for i, c in enumerate(stencil_ints):
        scaled = get(i) * weights[i]
        density = scaled if density is None else density + scaled
        for d in range(3):
            if c[d]:
                if sums[d] is None:
                    sums[d] = -scaled
                else:
                    sums[d] = sums[d] + scaled if c[d] > 0 else sums[d] - scaled
    return density, sums


def equilibria(density, velocity, wanted):
    square = velocity[0] * velocity[0] + velocity[1] * velocity[1] + velocity[2] * velocity[2]
    base = 1.0 - 1.5 * square
    for i in wanted:
        projected = None
        for d in range(3):
            if stencil_ints[i][d]:
                term = velocity[d] if stencil_ints[i][d] > 0 else -velocity[d]
                projected = term if projected is None else projected + term
        if projected is None:
            yield i, density * base
        else:
            yield i, density * (base + 3.0 * projected + 4.5 * projected * projected)


def interface(get, factor, wanted):
    density, sums = moments(get)
    velocity = [s / density for s in sums]
    return [(i, e + factor * (get(i) - e)) for i, e in equilibria(density, velocity, wanted)]


def iota(shape, dim):
    return lax.broadcasted_iota(jnp.int32, shape, dim)


def lane_map(ratio_in, ratio_out):
    rows = iota((128, 128), 0)
    cols = iota((128, 128), 1)
    return (rows // ratio_in == cols // ratio_out).astype(jnp.float32)


def kernel(
    sizes,
    pop,
    coarse,
    mask,
    inflow,
    dest,
    cell,
    vel,
    frac,
    drag,
    fine_out,
    coarse_out,
    parts,
    cbuf,
    cnext,
    fbuf,
    mid,
    force,
    cx_send,
    cx_recv,
    cy_send,
    cy_recv,
    cz_send,
    cz_recv,
    fx_send,
    fx_recv,
    fy_send,
    fy_recv,
    fz_send,
    fz_recv,
    part_sems,
    sems,
):
    n_x, n_y, n_z = sizes
    fx, fy, fz = pop.shape[1:]
    kx, ky, kz = coarse.shape[1:]
    names = ("gx", "gy", "gz")
    counts = (n_x, n_y, n_z)
    where_am_i = [lax.axis_index(a) for a in names]
    me = where_am_i[0]
    is_first = me == 0
    is_last = me == n_x - 1

    for ref in (cy_recv, cz_recv, fy_recv, fz_recv):
        ref[...] = jnp.full(ref.shape, closed, jnp.float32)

    barrier = pltpu.get_barrier_semaphore()
    expected = n_x - 1
    for step in range(1, n_x):
        pl.semaphore_signal(
            barrier, inc=1, device_id={"gx": lax.rem(me + step, n_x)}, device_id_type=MESH
        )
    for d in (1, 2):
        index = where_am_i[d]
        for side in (-1, 1):
            exists = index > 0 if side < 0 else index < counts[d] - 1

            @pl.when(exists)
            def _():
                pl.semaphore_signal(
                    barrier, inc=1, device_id={names[d]: index + side}, device_id_type=MESH
                )

            expected = expected + exists.astype(jnp.int32)

    own = parts.at[me]
    own[0:3, :] = vel[0, 0, 0]
    own[3:6, :] = frac[0, 0, 0]
    own[6:7, :] = drag[0, 0]
    own[7:8, :] = cell[0, 0].astype(jnp.float32)
    own[8:9, :] = dest[...].astype(jnp.float32)
    own[9:16, :] = jnp.zeros((7, dest.shape[1]), jnp.float32)
    pl.semaphore_wait(barrier, expected)

    part_copies = []
    for step in range(1, n_x):
        copy = pltpu.make_async_remote_copy(
            src_ref=own,
            dst_ref=own,
            send_sem=part_sems.at[0, step],
            recv_sem=part_sems.at[1, step],
            device_id={"gx": lax.rem(me + step, n_x)},
            device_id_type=MESH,
        )
        copy.start()
        part_copies.append(copy)

    def neighbour_copy(send, recv, slot, side, number, d):
        index = where_am_i[d]
        if d == 0:
            target = lax.rem(index + side + counts[d], counts[d])
        else:
            target = jnp.clip(index + side, 0, counts[d] - 1)
        return pltpu.make_async_remote_copy(
            src_ref=send.at[slot],
            dst_ref=recv.at[slot],
            send_sem=sems.at[0, number],
            recv_sem=sems.at[1, number],
            device_id={names[d]: target},
            device_id_type=MESH,
        )

    class Exchange:
        def __init__(self, send, recv, d, number):
            self.d = d
            self.copies = [
                neighbour_copy(send, recv, slot, side, number + slot, d)
                for slot, side in ((0, -1), (1, 1))
            ]

        def start(self):
            index, last = where_am_i[self.d], counts[self.d] - 1
            if self.d == 0:
                for copy in self.copies:
                    copy.start()
                return
            pl.when(index > 0)(self.copies[0].start)
            pl.when(index < last)(self.copies[1].start)

        def wait(self):
            index, last = where_am_i[self.d], counts[self.d] - 1
            if self.d == 0:
                for copy in self.copies:
                    copy.wait()
                return

            pl.when(index > 0)(self.copies[0].wait_send)
            pl.when(index < last)(self.copies[0].wait_recv)
            pl.when(index < last)(self.copies[1].wait_send)
            pl.when(index > 0)(self.copies[1].wait_recv)

    def refine(values):
        count = len(values)
        keep = iota((8, 128), 1) < kz
        flat = jnp.concatenate([jnp.where(keep, v, 0.0) for v in values], 0)
        rows = iota((128, 128), 0)
        cols = iota((128, 128), 1)
        spread = (rows == cols // 2).astype(jnp.float32)
        wide = jnp.dot(flat, spread, precision=HIGHEST, preferred_element_type=jnp.float32)
        row = iota((8, 128), 0)
        out = []
        for k in range(count):
            tile = wide[8 * k : 8 * k + 8]
            made = tile
            for by in range(1, 5):
                moved = pltpu.roll(tile, by, 0)
                made = jnp.where((row + 1) // 2 == by, moved, made)
            out.append(made)
        return out

    def late(get, send, number):
        made = interface(get, prolong_factor, groups[0, 1])
        return refine([v for _, v in made])

    cnext[...] = jnp.ones(cnext.shape, jnp.float32)
    for i in range(27):
        cnext[i, :, 0:ky, 0:kz] = coarse[i]

    density, sums = moments(lambda i: cnext[i])
    velocity = [s / density for s in sums]
    for i, e in equilibria(density, velocity, range(27)):
        n = cnext[i]
        cbuf[i] = n - (n - e) * (1.0 / tau_coarse)

    ahead = [pop[i, 0] + pop[i, 1] for i in range(27)]
    flat = jnp.concatenate(ahead, 0)
    gather_lanes = (iota((128, 128), 0) // 2 == iota((128, 128), 1)).astype(jnp.float32)
    narrow = jnp.dot(flat, gather_lanes, precision=HIGHEST, preferred_element_type=jnp.float32)
    row = iota((8, 128), 0)
    means = []
    for i in range(27):
        tile = narrow[8 * i : 8 * i + 8]
        tile = tile + pltpu.roll(tile, 7, 0)
        made = tile
        for by in range(1, 4):
            made = jnp.where(row == by, pltpu.roll(tile, 8 - by, 0), made)
        means.append(0.125 * made)
    restricted = interface(lambda i: means[i], restrict_factor, groups[0, -1])
    for k, (i, v) in enumerate(restricted):
        cx_send[0, k] = jnp.where(is_first, v, cbuf[i, 0])
    for k, i in enumerate(groups[0, 1]):
        cx_send[1, k] = cbuf[i, kx - 1]
    exchange_cx = Exchange(cx_send, cx_recv, 0, 0)
    exchange_cx.start()

    start_ghost = late(lambda i: cnext[i, kx - 1], None, 0)

    fluid = mask[...].astype(jnp.float32)
    open_cells = mask[...] > 0
    density, sums = moments(lambda i: pop[i])
    safe = density + (1.0 - fluid)
    inverse = 1.0 / safe
    cell_velocity = [s * inverse for s in sums]
    sample_from = jnp.concatenate(
        [v.reshape(fx * fy, fz).T for v in cell_velocity], 0
    )
    for copy in part_copies:
        copy.wait()
    total = None
    for source in range(n_x):
        block = parts[source]
        width = block.shape[1]
        where_cell = block[7:8].astype(jnp.int32)
        mine = block[8:9].astype(jnp.int32) == me
        first_row = jnp.where(mine, where_cell // fz, -1000)
        first_lane = where_cell % fz
        f_x, f_y, f_z = block[3:4], block[4:5], block[5:6]
        offset = iota((fx * fy, width), 0) - first_row
        across = (
            jnp.where(offset == 0, (1.0 - f_x) * (1.0 - f_y), 0.0)
            + jnp.where(offset == 1, (1.0 - f_x) * f_y, 0.0)
            + jnp.where(offset == fy, f_x * (1.0 - f_y), 0.0)
            + jnp.where(offset == fy + 1, f_x * f_y, 0.0)
        )
        offset = iota((fz, width), 0) - first_lane
        along = jnp.where(offset == 0, 1.0 - f_z, 0.0) + jnp.where(offset == 1, f_z, 0.0)
        lines = jnp.dot(
            sample_from, across, precision=HIGHEST, preferred_element_type=jnp.float32
        )
        pushes = []
        for d in range(3):
            sampled = jnp.sum(lines[d * fz : (d + 1) * fz] * along, axis=0, keepdims=True)
            impulse = block[6:7] * (block[d : d + 1] - sampled)
            pushes.append(along * impulse)
        added = lax.dot_general(
            across,
            jnp.concatenate(pushes, 0),
            (((1,), (1,)), ((), ())),
            precision=HIGHEST,
            preferred_element_type=jnp.float32,
        )
        total = added if total is None else total + added
    for d in range(3):
        force[d] = total[:, d * fz : (d + 1) * fz].reshape(fx, fy, fz)

    def fine_collide(get, density, sums, ghost, exchange, slot):
        safe = density + (1.0 - fluid)
        inverse = 1.0 / safe
        velocity = [(sums[d] + tau_fine * force[d]) * inverse for d in range(3)]
        for i, e in equilibria(safe, velocity, range(27)):
            n = get(i)
            fbuf[i] = jnp.where(open_cells, n - (n - e) * (1.0 / tau_fine), closed)
        for k, i in enumerate(groups[0, 1]):
            fx_send[slot, 1, k] = jnp.where(is_last, ghost[k], fbuf[i, fx - 1])
        for k, i in enumerate(groups[0, -1]):
            fx_send[slot, 0, k] = fbuf[i, 0]
        exchange.start()

    def shift_x(post, recv, stage, low, high, last):
        for i, c in enumerate(stencil_ints):
            if c[0] == 0:
                stage[i] = post[i]
            elif c[0] > 0:
                stage[i, 0] = low(i)
                for x in range(1, last + 1):
                    stage[i, x] = post[i, x - 1]
            else:
                stage[i, last] = high(i)
                for x in range(last):
                    stage[i, x] = post[i, x + 1]

    def send_y(stage, send, edge, exchange):
        for k, i in enumerate(groups[1, 1]):
            send[1, k] = stage[i, :, edge, :]
        for k, i in enumerate(groups[1, -1]):
            send[0, k] = stage[i, :, 0, :]
        exchange.start()

    def shift_y(stage, recv, edge, exchange):
        exchange.wait()
        row = iota(stage.shape[1:], 1)
        for side, slot, at, by in ((1, 1, 0, 1), (-1, 0, edge, 7)):
            for k, i in enumerate(groups[1, side]):
                stage[i] = jnp.where(
                    row == at, recv[slot, k][:, None, :], pltpu.roll(stage[i], by, 1)
                )

    def send_z(stage, send, edge, exchange):
        lane = iota(stage.shape[1:], 2)
        for side, slot, at in ((1, 1, edge), (-1, 0, 0)):
            packed = jnp.zeros(stage.shape[1:], jnp.float32)
            for k, i in enumerate(groups[2, side]):
                moved = pltpu.roll(stage[i], (k - at) % 128, 2)
                packed = jnp.where(lane == k, moved, packed)
            send[slot] = packed
        exchange.start()

    def shift_z(stage, recv, edge, exchange):
        exchange.wait()
        lane = iota(stage.shape[1:], 2)

        def get(i):
            side = stencil_ints[i][2]
            if side == 0:
                return stage[i]
            slot, at, by = (1, 0, 1) if side > 0 else (0, edge, 127)
            k = groups[2, side].index(i)
            column = pltpu.roll(recv[slot], (at - k) % 128, 2)
            return jnp.where(lane == at, column, pltpu.roll(stage[i], by, 2))

        return get

    fine_x = [Exchange(fx_send.at[s], fx_recv.at[s], 0, 6 + 6 * s) for s in (0, 1)]
    fine_y = [Exchange(fy_send.at[s], fy_recv.at[s], 1, 8 + 6 * s) for s in (0, 1)]
    fine_z = [Exchange(fz_send.at[s], fz_recv.at[s], 2, 10 + 6 * s) for s in (0, 1)]
    coarse_y = Exchange(cy_send, cy_recv, 1, 2)
    coarse_z = Exchange(cz_send, cz_recv, 2, 4)

    fine_collide(lambda i: pop[i], density, sums, start_ghost, fine_x[0], 0)

    exchange_cx.wait()
    speed = jnp.ones((8, 128), jnp.float32)
    cx_recv_low = {}
    zero = jnp.zeros((8, 128), jnp.float32)
    speed = inflow[...]
    for i, e in equilibria(1.0, [speed, zero, zero], groups[0, 1]):
        cx_recv_low[i] = jnp.where(is_first, e, cx_recv[1, groups[0, 1].index(i)])
    shift_x(
        cbuf, cx_recv, cnext, lambda i: cx_recv_low[i], lambda i: cx_recv[0, i], kx - 1
    )
    send_y(cnext, cy_send, ky - 1, coarse_y)

    def fine_x_phase(s):
        fine_x[s].wait()
        shift_x(
            fbuf,
            fx_recv,
            mid,
            lambda i: fx_recv[s, 1, i - 18],
            lambda i: jnp.where(is_last, fbuf[i, fx - 1], fx_recv[s, 0, i]),
            fx - 1,
        )
        send_y(mid, fy_send.at[s], fy - 1, fine_y[s])

    def finish_fine(s, out):
        get = shift_z(mid, fz_recv.at[s], fz - 1, fine_z[s])
        for i in range(27):
            v = get(i)
            v = jnp.where(v == closed, fbuf[26 - i], v)
            out[i] = jnp.where(open_cells, v, 0.0)

    fine_x_phase(0)
    shift_y(cnext, cy_recv, ky - 1, coarse_y)
    send_z(cnext, cz_send, kz - 1, coarse_z)
    shift_y(mid, fy_recv.at[0], fy - 1, fine_y[0])
    send_z(mid, fz_send.at[0], fz - 1, fine_z[0])

    get = shift_z(cnext, cz_recv, kz - 1, coarse_z)
    for i in range(27):
        v = get(i)
        v = jnp.where(v == closed, cbuf[26 - i], v)
        coarse_out[i] = v[:, 0:ky, 0:kz]
        cnext[i] = v
    half = jnp.ones((8, 128), jnp.float32)

    def halfway(i):
        layer = cnext[i, kx - 1, 0:ky, 0:kz]
        return 0.5 * (coarse[i, kx - 1] + layer)

    made = interface(halfway, prolong_factor, groups[0, 1])
    for k, (i, v) in enumerate(made):
        cx_send[0, k, 0:ky, 0:kz] = v
    late_ghost = refine([cx_send[0, k] for k in range(9)])

    finish_fine(0, fine_out)
    density, sums = moments(lambda i: fine_out[i])
    fine_collide(lambda i: fine_out[i], density, sums, late_ghost, fine_x[1], 1)
    fine_x_phase(1)
    shift_y(mid, fy_recv.at[1], fy - 1, fine_y[1])
    send_z(mid, fz_send.at[1], fz - 1, fine_z[1])
    finish_fine(1, fine_out)


def body(sizes, populations, coarse, mask, inflow, dest, cell, vel, frac, drag):
    fx, fy, fz = populations.shape[1:]
    kx, ky, kz = coarse.shape[1:]
    n_x = sizes[0]
    width = drag.shape[-1]
    padded = jnp.pad(inflow, ((0, 8 - ky), (0, 128 - kz)))
    vmem = pl.BlockSpec(memory_space=pltpu.VMEM)
    f32 = jnp.float32
    return pl.pallas_call(
        functools.partial(kernel, sizes),
        out_shape=(
            jax.ShapeDtypeStruct(populations.shape, f32),
            jax.ShapeDtypeStruct(coarse.shape, f32),
        ),
        in_specs=[vmem] * 9,
        out_specs=(vmem, vmem),
        scratch_shapes=[
            pltpu.VMEM((n_x, 16, width), f32),
            pltpu.VMEM((27, kx, 8, 128), f32),
            pltpu.VMEM((27, kx, 8, 128), f32),
            pltpu.VMEM((27, fx, fy, fz), f32),
            pltpu.VMEM((27, fx, fy, fz), f32),
            pltpu.VMEM((3, fx, fy, fz), f32),
            pltpu.VMEM((2, 9, 8, 128), f32),
            pltpu.VMEM((2, 9, 8, 128), f32),
            pltpu.VMEM((2, 9, kx, 128), f32),
            pltpu.VMEM((2, 9, kx, 128), f32),
            pltpu.VMEM((2, kx, 8, 128), f32),
            pltpu.VMEM((2, kx, 8, 128), f32),
            pltpu.VMEM((2, 2, 9, fy, fz), f32),
            pltpu.VMEM((2, 2, 9, fy, fz), f32),
            pltpu.VMEM((2, 2, 9, fx, fz), f32),
            pltpu.VMEM((2, 2, 9, fx, fz), f32),
            pltpu.VMEM((2, 2, fx, fy, fz), f32),
            pltpu.VMEM((2, 2, fx, fy, fz), f32),
            pltpu.SemaphoreType.DMA((2, n_x)),
            pltpu.SemaphoreType.DMA((2, 18)),
        ],
        compiler_params=pltpu.CompilerParams(collective_id=0, has_side_effects=True),
    )(populations, coarse, mask, padded, dest.reshape(1, width), cell, vel, frac, drag)


def solution(mesh):
    sizes = tuple(mesh.shape[a] for a in ("gx", "gy", "gz"))
    return jax.shard_map(
        functools.partial(body, sizes),
        mesh=mesh,
        in_specs=(
            P(None, "gx", "gy", "gz"),
            P(None, "gx", "gy", "gz"),
            P("gx", "gy", "gz"),
            P("gy", "gz"),
            P("gx", "gy", "gz", None, None),
            P("gx", "gy", "gz", None),
            P("gx", "gy", "gz", None, None),
            P("gx", "gy", "gz", None, None),
            P("gx", "gy", "gz", None),
        ),
        out_specs=(P(None, "gx", "gy", "gz"), P(None, "gx", "gy", "gz")),
        check_vma=False,
    )
```

```python
import functools

import jax
import jax.numpy as jnp
import numpy as np
from jax import lax
from jax.experimental import pallas as pl
from jax.experimental.pallas import tpu as pltpu
from jax.sharding import PartitionSpec as P

tau_fine = 1.3
tau_coarse = 0.9
stencil_ints = [
    (along_x, along_y, along_z)
    for along_x in (-1, 0, 1)
    for along_y in (-1, 0, 1)
    for along_z in (-1, 0, 1)
]
weights = [
    float(np.float32([8.0 / 27.0, 2.0 / 27.0, 1.0 / 54.0, 1.0 / 216.0][sum(map(abs, c))]))
    for c in stencil_ints
]
prolong_factor = (tau_fine - 1.0) / (2.0 * tau_coarse)
restrict_factor = 2.0 * (tau_coarse - 1.0) / tau_fine
closed = -3.0e38
groups = {
    (dim, side): [i for i, c in enumerate(stencil_ints) if c[dim] == side]
    for dim in range(3)
    for side in (-1, 1)
}
MESH = pl.DeviceIdType.MESH
HIGHEST = lax.Precision.HIGHEST


def moments(get):
    density = None
    sums = [None, None, None]
    for i, c in enumerate(stencil_ints):
        scaled = get(i) * weights[i]
        density = scaled if density is None else density + scaled
        for d in range(3):
            if c[d]:
                if sums[d] is None:
                    sums[d] = -scaled
                else:
                    sums[d] = sums[d] + scaled if c[d] > 0 else sums[d] - scaled
    return density, sums


def equilibria(density, velocity, wanted):
    square = velocity[0] * velocity[0] + velocity[1] * velocity[1] + velocity[2] * velocity[2]
    base = 1.0 - 1.5 * square
    for i in wanted:
        projected = None
        for d in range(3):
            if stencil_ints[i][d]:
                term = velocity[d] if stencil_ints[i][d] > 0 else -velocity[d]
                projected = term if projected is None else projected + term
        if projected is None:
            yield i, density * base
        else:
            yield i, density * (base + 3.0 * projected + 4.5 * projected * projected)


def interface(get, factor, wanted):
    density, sums = moments(get)
    velocity = [s / density for s in sums]
    return [(i, e + factor * (get(i) - e)) for i, e in equilibria(density, velocity, wanted)]


def iota(shape, dim):
    return lax.broadcasted_iota(jnp.int32, shape, dim)


def lane_map(ratio_in, ratio_out):
    rows = iota((128, 128), 0)
    cols = iota((128, 128), 1)
    return (rows // ratio_in == cols // ratio_out).astype(jnp.float32)


def kernel(
    sizes,
    pop,
    coarse,
    mask,
    inflow,
    dest,
    cell,
    vel,
    frac,
    drag,
    fine_out,
    coarse_out,
    parts,
    cbuf,
    cnext,
    fbuf,
    mid,
    force,
    inlet,
    cx_send,
    cx_recv,
    cy_send,
    cy_recv,
    cz_send,
    cz_recv,
    fx_send,
    fx_recv,
    fy_send,
    fy_recv,
    fz_send,
    fz_recv,
    part_sems,
    sems,
):
    n_x, n_y, n_z = sizes
    fx, fy, fz = pop.shape[1:]
    kx, ky, kz = coarse.shape[1:]
    names = ("gx", "gy", "gz")
    counts = (n_x, n_y, n_z)
    where_am_i = [lax.axis_index(a) for a in names]
    me = where_am_i[0]
    is_first = me == 0
    is_last = me == n_x - 1

    for ref in (cy_recv, cz_recv, fy_recv, fz_recv):
        ref[...] = jnp.full(ref.shape, closed, jnp.float32)

    barrier = pltpu.get_barrier_semaphore()
    expected = n_x - 1
    for step in range(1, n_x):
        pl.semaphore_signal(
            barrier, inc=1, device_id={"gx": lax.rem(me + step, n_x)}, device_id_type=MESH
        )
    for d in (1, 2):
        index = where_am_i[d]
        for side in (-1, 1):
            exists = index > 0 if side < 0 else index < counts[d] - 1

            @pl.when(exists)
            def _():
                pl.semaphore_signal(
                    barrier, inc=1, device_id={names[d]: index + side}, device_id_type=MESH
                )

            expected = expected + exists.astype(jnp.int32)

    own = parts.at[me]
    for d in range(3):
        own[d : d + 1, :] = vel[d]
        own[3 + d : 4 + d, :] = frac[d]
    own[6:7, :] = drag[0, 0]
    own[7:8, :] = cell[0, 0].astype(jnp.float32)
    own[8:9, :] = dest[...].astype(jnp.float32)
    own[9:16, :] = jnp.zeros((7, dest.shape[1]), jnp.float32)
    pl.semaphore_wait(barrier, expected)

    part_copies = []
    for step in range(1, n_x):
        copy = pltpu.make_async_remote_copy(
            src_ref=own,
            dst_ref=own,
            send_sem=part_sems.at[0, step],
            recv_sem=part_sems.at[1, step],
            device_id={"gx": lax.rem(me + step, n_x)},
            device_id_type=MESH,
        )
        copy.start()
        part_copies.append(copy)

    def neighbour_copy(send, recv, slot, side, number, d):
        index = where_am_i[d]
        if d == 0:
            target = lax.rem(index + side + counts[d], counts[d])
        else:
            target = jnp.clip(index + side, 0, counts[d] - 1)
        return pltpu.make_async_remote_copy(
            src_ref=send.at[slot],
            dst_ref=recv.at[slot],
            send_sem=sems.at[0, number],
            recv_sem=sems.at[1, number],
            device_id={names[d]: target},
            device_id_type=MESH,
        )

    class Exchange:
        def __init__(self, send, recv, d, number):
            self.d = d
            self.copies = [
                neighbour_copy(send, recv, slot, side, number + slot, d)
                for slot, side in ((0, -1), (1, 1))
            ]

        def start(self):
            index, last = where_am_i[self.d], counts[self.d] - 1
            if self.d == 0:
                for copy in self.copies:
                    copy.start()
                return
            pl.when(index > 0)(self.copies[0].start)
            pl.when(index < last)(self.copies[1].start)

        def wait(self):
            index, last = where_am_i[self.d], counts[self.d] - 1
            if self.d == 0:
                for copy in self.copies:
                    copy.wait()
                return

            pl.when(index > 0)(self.copies[0].wait_send)
            pl.when(index < last)(self.copies[0].wait_recv)
            pl.when(index < last)(self.copies[1].wait_send)
            pl.when(index > 0)(self.copies[1].wait_recv)

    def refine(values):
        count = len(values)
        keep = iota((8, 128), 1) < kz
        flat = jnp.concatenate([jnp.where(keep, v, 0.0) for v in values], 0)
        rows = iota((128, 128), 0)
        cols = iota((128, 128), 1)
        spread = (rows == cols // 2).astype(jnp.float32)
        wide = jnp.dot(flat, spread, precision=HIGHEST, preferred_element_type=jnp.float32)
        row = iota((8, 128), 0)
        out = []
        for k in range(count):
            tile = wide[8 * k : 8 * k + 8]
            made = tile
            for by in range(1, 5):
                moved = pltpu.roll(tile, by, 0)
                made = jnp.where((row + 1) // 2 == by, moved, made)
            out.append(made)
        return out

    def late(get, send, number):
        made = interface(get, prolong_factor, groups[0, 1])
        return refine([v for _, v in made])

    cnext[...] = jnp.ones(cnext.shape, jnp.float32)
    for i in range(27):
        cnext[i, :, 0:ky, 0:kz] = coarse[i]

    density, sums = moments(lambda i: cnext[i])
    velocity = [s / density for s in sums]
    for i, e in equilibria(density, velocity, range(27)):
        n = cnext[i]
        cbuf[i] = n - (n - e) * (1.0 / tau_coarse)

    ahead = [pop[i, 0] + pop[i, 1] for i in range(27)]
    flat = jnp.concatenate(ahead, 0)
    gather_lanes = (iota((128, 128), 0) // 2 == iota((128, 128), 1)).astype(jnp.float32)
    narrow = jnp.dot(flat, gather_lanes, precision=HIGHEST, preferred_element_type=jnp.float32)
    row = iota((8, 128), 0)
    means = []
    for i in range(27):
        tile = narrow[8 * i : 8 * i + 8]
        tile = tile + pltpu.roll(tile, 7, 0)
        made = tile
        for by in range(1, 4):
            made = jnp.where(row == by, pltpu.roll(tile, 8 - by, 0), made)
        means.append(0.125 * made)
    restricted = interface(lambda i: means[i], restrict_factor, groups[0, -1])
    for k, (i, v) in enumerate(restricted):
        cx_send[0, k] = jnp.where(is_first, v, cbuf[i, 0])
    for k, i in enumerate(groups[0, 1]):
        cx_send[1, k] = cbuf[i, kx - 1]
    exchange_cx = Exchange(cx_send, cx_recv, 0, 0)
    exchange_cx.start()

    start_ghost = late(lambda i: cnext[i, kx - 1], None, 0)

    fluid = mask[...].astype(jnp.float32)
    open_cells = mask[...] > 0
    density, sums = moments(lambda i: pop[i])
    safe = density + (1.0 - fluid)
    inverse = 1.0 / safe
    cell_velocity = [s * inverse for s in sums]
    sample_from = jnp.concatenate(
        [v.reshape(fx * fy, fz).T for v in cell_velocity], 0
    )
    for copy in part_copies:
        copy.wait()
    total = None
    for first in range(0, n_x, 4):
        block = jnp.concatenate([parts[s] for s in range(first, min(first + 4, n_x))], 1)
        width = block.shape[1]
        where_cell = block[7:8].astype(jnp.int32)
        mine = block[8:9].astype(jnp.int32) == me
        first_row = jnp.where(mine, where_cell // fz, -1000)
        first_lane = where_cell % fz
        f_x, f_y, f_z = block[3:4], block[4:5], block[5:6]
        offset = iota((fx * fy, width), 0) - first_row
        across = (
            jnp.where(offset == 0, (1.0 - f_x) * (1.0 - f_y), 0.0)
            + jnp.where(offset == 1, (1.0 - f_x) * f_y, 0.0)
            + jnp.where(offset == fy, f_x * (1.0 - f_y), 0.0)
            + jnp.where(offset == fy + 1, f_x * f_y, 0.0)
        )
        offset = iota((fz, width), 0) - first_lane
        along = jnp.where(offset == 0, 1.0 - f_z, 0.0) + jnp.where(offset == 1, f_z, 0.0)
        lines = jnp.dot(
            sample_from, across, precision=HIGHEST, preferred_element_type=jnp.float32
        )
        pushes = []
        for d in range(3):
            sampled = jnp.sum(lines[d * fz : (d + 1) * fz] * along, axis=0, keepdims=True)
            impulse = block[6:7] * (block[d : d + 1] - sampled)
            pushes.append(along * impulse)
        added = lax.dot_general(
            across,
            jnp.concatenate(pushes, 0),
            (((1,), (1,)), ((), ())),
            precision=HIGHEST,
            preferred_element_type=jnp.float32,
        )
        total = added if total is None else total + added
    for d in range(3):
        force[d] = total[:, d * fz : (d + 1) * fz].reshape(fx, fy, fz)

    def fine_collide(get, density, sums, ghost, exchange, slot):
        safe = density + (1.0 - fluid)
        inverse = 1.0 / safe
        velocity = [(sums[d] + tau_fine * force[d]) * inverse for d in range(3)]
        for i, e in equilibria(safe, velocity, range(27)):
            n = get(i)
            fbuf[i] = jnp.where(open_cells, n - (n - e) * (1.0 / tau_fine), closed)
        for k, i in enumerate(groups[0, 1]):
            fx_send[slot, 1, k] = jnp.where(is_last, ghost[k], fbuf[i, fx - 1])
        for k, i in enumerate(groups[0, -1]):
            fx_send[slot, 0, k] = fbuf[i, 0]
        exchange.start()

    def shift_x(post, recv, stage, low, high, last):
        for i, c in enumerate(stencil_ints):
            if c[0] == 0:
                stage[i] = post[i]
            elif c[0] > 0:
                stage[i, 0] = low(i)
                for x in range(1, last + 1):
                    stage[i, x] = post[i, x - 1]
            else:
                stage[i, last] = high(i)
                for x in range(last):
                    stage[i, x] = post[i, x + 1]

    def send_y(stage, send, edge, exchange):
        for k, i in enumerate(groups[1, 1]):
            send[1, k] = stage[i, :, edge, :]
        for k, i in enumerate(groups[1, -1]):
            send[0, k] = stage[i, :, 0, :]
        exchange.start()

    def shift_y(stage, recv, edge, exchange):
        exchange.wait()
        row = iota(stage.shape[1:], 1)
        for side, slot, at, by in ((1, 1, 0, 1), (-1, 0, edge, 7)):
            for k, i in enumerate(groups[1, side]):
                stage[i] = jnp.where(
                    row == at, recv[slot, k][:, None, :], pltpu.roll(stage[i], by, 1)
                )

    def send_z(stage, send, edge, exchange):
        lane = iota(stage.shape[1:], 2)
        for side, slot, at in ((1, 1, edge), (-1, 0, 0)):
            packed = jnp.zeros(stage.shape[1:], jnp.float32)
            for k, i in enumerate(groups[2, side]):
                moved = pltpu.roll(stage[i], (k - at) % 128, 2)
                packed = jnp.where(lane == k, moved, packed)
            send[slot] = packed
        exchange.start()

    def shift_z(stage, recv, edge, exchange):
        exchange.wait()
        lane = iota(stage.shape[1:], 2)

        def get(i):
            side = stencil_ints[i][2]
            if side == 0:
                return stage[i]
            slot, at, by = (1, 0, 1) if side > 0 else (0, edge, 127)
            k = groups[2, side].index(i)
            column = pltpu.roll(recv[slot], (at - k) % 128, 2)
            return jnp.where(lane == at, column, pltpu.roll(stage[i], by, 2))

        return get

    fine_x = [Exchange(fx_send.at[s], fx_recv.at[s], 0, 6 + 6 * s) for s in (0, 1)]
    fine_y = [Exchange(fy_send.at[s], fy_recv.at[s], 1, 8 + 6 * s) for s in (0, 1)]
    fine_z = [Exchange(fz_send.at[s], fz_recv.at[s], 2, 10 + 6 * s) for s in (0, 1)]
    coarse_y = Exchange(cy_send, cy_recv, 1, 2)
    coarse_z = Exchange(cz_send, cz_recv, 2, 4)

    fine_collide(lambda i: pop[i], density, sums, start_ghost, fine_x[0], 0)

    exchange_cx.wait()
    cx_recv_low = {}
    zero = jnp.zeros((8, 128), jnp.float32)
    inlet[...] = zero
    inlet[0:ky, 0:kz] = inflow[...]
    speed = inlet[...]
    for i, e in equilibria(1.0, [speed, zero, zero], groups[0, 1]):
        cx_recv_low[i] = jnp.where(is_first, e, cx_recv[1, groups[0, 1].index(i)])
    shift_x(
        cbuf, cx_recv, cnext, lambda i: cx_recv_low[i], lambda i: cx_recv[0, i], kx - 1
    )
    send_y(cnext, cy_send, ky - 1, coarse_y)

    def fine_x_phase(s):
        fine_x[s].wait()
        shift_x(
            fbuf,
            fx_recv,
            mid,
            lambda i: fx_recv[s, 1, i - 18],
            lambda i: jnp.where(is_last, fbuf[i, fx - 1], fx_recv[s, 0, i]),
            fx - 1,
        )
        send_y(mid, fy_send.at[s], fy - 1, fine_y[s])

    def finish_fine(s, out):
        get = shift_z(mid, fz_recv.at[s], fz - 1, fine_z[s])
        for i in range(27):
            v = get(i)
            v = jnp.where(v == closed, fbuf[26 - i], v)
            out[i] = jnp.where(open_cells, v, 0.0)

    fine_x_phase(0)
    shift_y(cnext, cy_recv, ky - 1, coarse_y)
    send_z(cnext, cz_send, kz - 1, coarse_z)
    shift_y(mid, fy_recv.at[0], fy - 1, fine_y[0])
    send_z(mid, fz_send.at[0], fz - 1, fine_z[0])

    get = shift_z(cnext, cz_recv, kz - 1, coarse_z)
    for i in range(27):
        v = get(i)
        v = jnp.where(v == closed, cbuf[26 - i], v)
        coarse_out[i] = v[:, 0:ky, 0:kz]
        cnext[i] = v

    def halfway(i):
        layer = cnext[i, kx - 1, 0:ky, 0:kz]
        return 0.5 * (coarse[i, kx - 1] + layer)

    made = interface(halfway, prolong_factor, groups[0, 1])
    for k, (i, v) in enumerate(made):
        cx_send[0, k, 0:ky, 0:kz] = v
    late_ghost = refine([cx_send[0, k] for k in range(9)])

    finish_fine(0, fine_out)
    density, sums = moments(lambda i: fine_out[i])
    fine_collide(lambda i: fine_out[i], density, sums, late_ghost, fine_x[1], 1)
    fine_x_phase(1)
    shift_y(mid, fy_recv.at[1], fy - 1, fine_y[1])
    send_z(mid, fz_send.at[1], fz - 1, fine_z[1])
    finish_fine(1, fine_out)


def body(sizes, populations, coarse, mask, inflow, dest, cell, vel, frac, drag):
    fx, fy, fz = populations.shape[1:]
    kx, ky, kz = coarse.shape[1:]
    n_x = sizes[0]
    width = drag.shape[-1]
    vmem = pl.BlockSpec(memory_space=pltpu.VMEM)
    f32 = jnp.float32
    return pl.pallas_call(
        functools.partial(kernel, sizes),
        out_shape=(
            jax.ShapeDtypeStruct(populations.shape, f32),
            jax.ShapeDtypeStruct(coarse.shape, f32),
        ),
        in_specs=[vmem] * 9,
        out_specs=(vmem, vmem),
        scratch_shapes=[
            pltpu.VMEM((n_x, 16, width), f32),
            pltpu.VMEM((27, kx, 8, 128), f32),
            pltpu.VMEM((27, kx, 8, 128), f32),
            pltpu.VMEM((27, fx, fy, fz), f32),
            pltpu.VMEM((27, fx, fy, fz), f32),
            pltpu.VMEM((3, fx, fy, fz), f32),
            pltpu.VMEM((8, 128), f32),
            pltpu.VMEM((2, 9, 8, 128), f32),
            pltpu.VMEM((2, 9, 8, 128), f32),
            pltpu.VMEM((2, 9, kx, 128), f32),
            pltpu.VMEM((2, 9, kx, 128), f32),
            pltpu.VMEM((2, kx, 8, 128), f32),
            pltpu.VMEM((2, kx, 8, 128), f32),
            pltpu.VMEM((2, 2, 9, fy, fz), f32),
            pltpu.VMEM((2, 2, 9, fy, fz), f32),
            pltpu.VMEM((2, 2, 9, fx, fz), f32),
            pltpu.VMEM((2, 2, 9, fx, fz), f32),
            pltpu.VMEM((2, 2, fx, fy, fz), f32),
            pltpu.VMEM((2, 2, fx, fy, fz), f32),
            pltpu.SemaphoreType.DMA((2, n_x)),
            pltpu.SemaphoreType.DMA((2, 18)),
        ],
        compiler_params=pltpu.CompilerParams(collective_id=0, has_side_effects=True),
    )(populations, coarse, mask, inflow, dest.reshape(1, width), cell, vel.reshape(3, 1, width), frac.reshape(3, 1, width), drag)


def solution(mesh):
    sizes = tuple(mesh.shape[a] for a in ("gx", "gy", "gz"))
    return jax.shard_map(
        functools.partial(body, sizes),
        mesh=mesh,
        in_specs=(
            P(None, "gx", "gy", "gz"),
            P(None, "gx", "gy", "gz"),
            P("gx", "gy", "gz"),
            P("gy", "gz"),
            P("gx", "gy", "gz", None, None),
            P("gx", "gy", "gz", None),
            P("gx", "gy", "gz", None, None),
            P("gx", "gy", "gz", None, None),
            P("gx", "gy", "gz", None),
        ),
        out_specs=(P(None, "gx", "gy", "gz"), P(None, "gx", "gy", "gz")),
        check_vma=False,
    )
```
